1024 devices in a mesh: dp: 64 (over z, core), mp: 16 (over x, y).
Axes of the slice: x: 4, y: 4, z: 32, core: 2. Of those that a mesh axis runs over, the one named last changes fastest.
Arguments:
- block_input: bfloat16 [32768, 6144], P('dp', 'mp'), may hold values from -6 to 6
- prenorm_gain: float32 [6144], P('mp'), may hold values from 0.5 to 1.5
- weight: bfloat16 [6144, 3072], P('mp', 'dp'), may hold values from -0.078125 to 0.078125
- query: bfloat16 [32768, 3072], P('dp'), may hold values from -6 to 6
- grad_normed: bfloat16 [32768, 3072], P('dp'), may hold values from -6 to 6
- qk_gain: float32 [128], replicated, may hold values from 0.5 to 1.5
Outputs:
- input_gradient: bfloat16 [32768, 6144], P('dp', 'mp')
- grad_weight: float32 [6144, 3072], P('mp', 'dp')
- prenorm_gain_gradient: float32 [6144], P('mp')
- grad_qk_gain: float32 [128], replicated
The draws below stay inside these ranges and needn't reach their ends.
All inputs are finite; a program needn't handle non-finite values.
Results may differ from the reference program's by a relative error of at most 0.0049.
Values may be sent and summed in bfloat16 or wider, within the bound.
No kernel may reach another device: no remote copies, remote signals or barrier semaphores. Data moves between devices by JAX's collectives and lax.ppermute only.
A program may use at most 64 MiB of HBM per device.

```python
import jax
import jax.numpy as jnp
from jax import lax

D = 6144
HEADS = 24
HEAD_DIM = 128
WIDTH = 3072
TOKENS = 32768


def level_of(rng, shape, shards, low, largest):
    gain = 1.0
    for axis_at, blocks in shards:
        steps = jax.random.uniform(jax.random.fold_in(jax.random.fold_in(rng, 6), axis_at), (blocks,), jnp.float32, low / len(shards), largest / len(shards))
        gain = gain * jnp.repeat(jnp.exp(steps), shape[axis_at] // blocks).reshape((-1,) + (1,) * (len(shape) - 1 - axis_at))
    return gain


def centred(rng, dims, width, limit, cuts=(), kind=jnp.bfloat16):
    entries = width * jax.random.normal(rng, dims, jnp.float32)
    if cuts:
        entries = entries * level_of(rng, dims, cuts, -0.22, 0.18)
    return jnp.clip(entries, -limit, limit).astype(kind)


def setup_inputs(seed: int = 0) -> dict:
    splits = jax.random.split(jax.random.key(seed), 7)
    block_input = centred(splits[0], (TOKENS, D), 1.0, 6.0, ((0, 64), (1, 16)))
    prenorm_gain = jnp.clip(1.0 + 0.1 * jax.random.normal(splits[1], (D,), jnp.float32), 0.5, 1.5)
    weight = centred(splits[2], (D, WIDTH), D ** -0.5, 0.078125, ((0, 16), (1, 64)))
    query = centred(splits[3], (TOKENS, WIDTH), 1.0, 6.0, ((0, 64),))
    grad_normed = centred(splits[4], (TOKENS, WIDTH), 1.0, 6.0, ((0, 64),))
    qk_gain = jnp.clip(1.0 + 0.1 * jax.random.normal(splits[5], (HEAD_DIM,), jnp.float32), 0.5, 1.5)
    return {"block_input": block_input, "prenorm_gain": prenorm_gain, "weight": weight, "query": query, "grad_normed": grad_normed, "qk_gain": qk_gain}


EPS = 1e-06

def reference(block_input, prenorm_gain, weight, query, grad_normed, qk_gain):
    input_wide_float = block_input.astype(jnp.float32)
    row_average = lax.optimization_barrier(jnp.mean(input_wide_float, axis=1, keepdims=True))
    variance = lax.optimization_barrier(jnp.mean(input_wide_float * input_wide_float, axis=1, keepdims=True)) - row_average * row_average
    reciprocal_deviation = lax.rsqrt(variance + EPS)
    standardized_input = (input_wide_float - row_average) * reciprocal_deviation
    prenormed_rows = (standardized_input * prenorm_gain).astype(jnp.bfloat16)
    q_float = query.astype(jnp.float32).reshape(TOKENS, HEADS, HEAD_DIM)
    q_mean = lax.optimization_barrier(jnp.mean(q_float, axis=2, keepdims=True))
    q_var = lax.optimization_barrier(jnp.mean(q_float * q_float, axis=2, keepdims=True)) - q_mean * q_mean
    q_inv = lax.rsqrt(q_var + EPS)
    qhat = (q_float - q_mean) * q_inv
    upstream = grad_normed.astype(jnp.float32).reshape(TOKENS, HEADS, HEAD_DIM)
    dqhat = upstream * qk_gain
    grad_query = q_inv * (dqhat - lax.optimization_barrier(jnp.mean(dqhat, axis=2, keepdims=True)) - qhat * lax.optimization_barrier(jnp.mean(dqhat * qhat, axis=2, keepdims=True)))
    grad_query = grad_query.reshape(TOKENS, WIDTH).astype(jnp.bfloat16)
    grad_qk_gain = lax.optimization_barrier(jnp.sum(upstream * qhat, axis=(0, 1)))
    grad_weight = jnp.dot(prenormed_rows.T, grad_query, preferred_element_type=jnp.float32)
    gradient_prenormed_input = jnp.dot(grad_query, weight.T, preferred_element_type=jnp.float32)
    prenorm_gain_gradient = lax.optimization_barrier(jnp.sum(gradient_prenormed_input * standardized_input, axis=0))
    standardized_gradient = gradient_prenormed_input * prenorm_gain
    input_gradient = reciprocal_deviation * (standardized_gradient - lax.optimization_barrier(jnp.mean(standardized_gradient, axis=1, keepdims=True)) - standardized_input * lax.optimization_barrier(jnp.mean(standardized_gradient * standardized_input, axis=1, keepdims=True)))
    return (input_gradient.astype(jnp.bfloat16), grad_weight, prenorm_gain_gradient, grad_qk_gain)
```

```python
import jax
import jax.numpy as jnp
from jax import lax
from jax.experimental import pallas as pl
from jax.experimental.pallas import tpu as pltpu
from jax.sharding import Mesh
from jax.sharding import PartitionSpec as P

D = 6144
EPS = 1e-06
HEAD = 128
FAR, NEAR = 8, 4
COLS = 48
MP = ("x", "y")
DP = ("far", "near", "core")


def qk_kernel(core_ref, query_ref, grad_ref, gain_ref, out_ref, gain_grad_ref, rows_ref):
    @pl.when(pl.program_id(0) == 0)
    def _():
        gain_grad_ref[...] = jnp.zeros_like(gain_grad_ref)

    core = core_ref[0]
    gain = gain_ref[...]
    scale = 1.0 / HEAD

    def three_heads(group, total):
        for j in range(3):
            cols = pl.ds(pl.multiple_of(group * 384 + j * HEAD, HEAD), HEAD)
            q = query_ref[:, cols].astype(jnp.float32)
            upstream = grad_ref[:, cols].astype(jnp.float32)
            mean = jnp.sum(q, axis=1, keepdims=True) * scale
            var = jnp.sum(q * q, axis=1, keepdims=True) * scale - mean * mean
            inv = lax.rsqrt(var + EPS)
            qhat = (q - mean) * inv
            dqhat = upstream * gain
            mean_d = jnp.sum(dqhat, axis=1, keepdims=True) * scale
            mean_c = jnp.sum(dqhat * qhat, axis=1, keepdims=True) * scale
            rows_ref[:, j * HEAD : (j + 1) * HEAD] = (
                inv * (dqhat - mean_d - qhat * mean_c)
            ).astype(jnp.bfloat16)
            total = total + jnp.sum((upstream * qhat).reshape(-1, 8, HEAD), axis=0)
        turned = jnp.transpose(rows_ref[...])
        for b in range(8):
            out_ref[(b % 2 + core) % 2, b // 2, group] = turned[COLS * b : COLS * (b + 1)]
        return total

    zero = jnp.zeros((8, HEAD), jnp.float32)
    gain_grad_ref[...] += lax.fori_loop(0, FAR, three_heads, zero)


def qk_backward(core, query, grad_normed, qk_gain):
    tokens, width = query.shape
    block = 128
    return pl.pallas_call(
        qk_kernel,
        grid=(tokens // block,),
        in_specs=[
            pl.BlockSpec(memory_space=pltpu.SMEM),
            pl.BlockSpec((block, width), lambda i: (i, 0)),
            pl.BlockSpec((block, width), lambda i: (i, 0)),
            pl.BlockSpec((1, HEAD), lambda i: (0, 0)),
        ],
        out_specs=[
            pl.BlockSpec((2, NEAR, FAR, COLS, block), lambda i: (0, 0, 0, 0, i)),
            pl.BlockSpec((8, HEAD), lambda i: (0, 0)),
        ],
        out_shape=[
            jax.ShapeDtypeStruct((2, NEAR, FAR, COLS, tokens), jnp.bfloat16),
            jax.ShapeDtypeStruct((8, HEAD), jnp.float32),
        ],
        scratch_shapes=[pltpu.VMEM((block, 3 * HEAD), jnp.bfloat16)],
        compiler_params=pltpu.CompilerParams(dimension_semantics=("arbitrary",)),
        cost_estimate=pl.CostEstimate(
            flops=60_000_000, bytes_accessed=9_500_000, transcendentals=12288
        ),
    )(core, query, grad_normed, qk_gain.reshape(1, HEAD))


def exchange(x, axes):
    return lax.all_to_all(x, axes, 0, 0, tiled=True)


def shared_by(x, axes):
    copies = jnp.broadcast_to(x[None], (lax.axis_size(axes), *x.shape))
    return exchange(copies, axes)


def swapped(x):
    return lax.ppermute(x, "core", [(0, 1), (1, 0)])


def shards(block_input, prenorm_gain, weight, query, grad_normed, qk_gain):
    tokens, rows = block_input.shape
    core = lax.axis_index("core").astype(jnp.int32).reshape(1)

    own = shared_by(shared_by(weight.T, "far"), "near").reshape(-1, rows)
    other = swapped(own)

    x = block_input.T.astype(jnp.float32)
    sums = jnp.concatenate([jnp.sum(x, axis=0), jnp.sum(x * x, axis=0)]).reshape(8, 128)
    sums = jnp.sum(shared_by(sums, MP), axis=0).reshape(2, tokens)

    grad_query, qk_partial = qk_backward(core, query, grad_normed, qk_gain)

    mean = sums[0:1] / D
    inv = lax.rsqrt(sums[1:2] / D - mean * mean + EPS)
    xhat = (x - mean) * inv
    gain = prenorm_gain[:, None]
    normed = (xhat * gain).astype(jnp.bfloat16)

    def weight_part(k):
        return lax.dot_general(
            grad_query[k].reshape(-1, tokens), normed, (((1,), (1,)), ((), ())),
            preferred_element_type=jnp.float32,
        )

    from_core = swapped(weight_part(1).astype(jnp.bfloat16))
    part = weight_part(0) + from_core.astype(jnp.float32)
    part = part.astype(jnp.bfloat16).reshape(NEAR, FAR, COLS, rows)
    part = jnp.sum(exchange(part, "near").astype(jnp.float32), axis=0)
    part = exchange(part.astype(jnp.bfloat16), "far").astype(jnp.float32)
    grad_weight = jnp.sum(part, axis=0).T

    def input_part(w, k):
        return lax.dot_general(
            w, grad_query[k].reshape(-1, tokens), (((0,), (0,)), ((), ())),
            preferred_element_type=jnp.float32,
        )

    grad = input_part(own, 0) + input_part(other, 1)
    slope = grad * gain
    slopes = jnp.concatenate([jnp.sum(slope, axis=0), jnp.sum(slope * xhat, axis=0)])
    slopes = jnp.sum(shared_by(slopes.reshape(8, 128), MP), axis=0).reshape(2, tokens) / D
    input_gradient = (inv * (slope - slopes[0:1] - xhat * slopes[1:2])).astype(jnp.bfloat16).T

    gains = jnp.concatenate([jnp.sum(grad * xhat, axis=1), jnp.sum(qk_partial, axis=0)])
    gains = gains.reshape(4, 128)
    gains = gains + swapped(gains)
    gains = jnp.sum(shared_by(gains, "near"), axis=0)
    gains = jnp.sum(shared_by(gains, "far"), axis=0).reshape(-1)
    return (input_gradient, grad_weight, gains[:rows], gains[rows:])


def solution(mesh):
    finer = Mesh(
        mesh.devices.reshape(FAR, NEAR, 2, 4, 4), (*DP, *MP)
    )
    in_specs = (P(DP, MP), P(MP), P(MP, DP), P(DP, None), P(DP, None), P())
    out_specs = (P(DP, MP), P(MP, DP), P(MP), P())
    return jax.shard_map(
        shards, mesh=finer, in_specs=in_specs, out_specs=out_specs, check_vma=False
    )
```

```python
import jax
import jax.numpy as jnp
from jax import lax
from jax.experimental import pallas as pl
from jax.experimental.pallas import tpu as pltpu
from jax.sharding import Mesh
from jax.sharding import PartitionSpec as P


D = 6144
EPS = 1e-06
HEAD = 128
FAR, NEAR = 8, 4
COLS = 48
MP = ("x", "y")
DP = ("far", "near", "core")


def qk_kernel(
    core_ref, query_ref, grad_ref, gain_ref, own_ref, other_ref, gain_grad_ref, rows_ref
):
    @pl.when(pl.program_id(0) == 0)
    def _():
        gain_grad_ref[...] = jnp.zeros_like(gain_grad_ref)

    core = core_ref[0]
    gain = gain_ref[...]
    scale = 1.0 / HEAD

    def three_heads(group, total):
        for j in range(3):
            cols = pl.ds(pl.multiple_of(group * 384 + j * HEAD, HEAD), HEAD)
            q = query_ref[:, cols].astype(jnp.float32)
            upstream = grad_ref[:, cols].astype(jnp.float32)
            mean = jnp.sum(q, axis=1, keepdims=True) * scale
            var = jnp.sum(q * q, axis=1, keepdims=True) * scale - mean * mean
            inv = lax.rsqrt(var + EPS)
            qhat = (q - mean) * inv
            dqhat = upstream * gain
            mean_d = jnp.sum(dqhat, axis=1, keepdims=True) * scale
            mean_c = jnp.sum(dqhat * qhat, axis=1, keepdims=True) * scale
            rows_ref[:, j * HEAD : (j + 1) * HEAD] = (
                inv * (dqhat - mean_d - qhat * mean_c)
            ).astype(jnp.bfloat16)
            total = total + jnp.sum((upstream * qhat).reshape(-1, 8, HEAD), axis=0)
        turned = jnp.transpose(rows_ref[...])
        for parity, (even_ref, odd_ref) in enumerate(((own_ref, other_ref), (other_ref, own_ref))):

            @pl.when(core == parity)
            def _():
                for b in range(8):
                    to_ref = odd_ref if b % 2 else even_ref
                    to_ref[b // 2, group] = turned[COLS * b : COLS * (b + 1)]

        return total

    zero = jnp.zeros((8, HEAD), jnp.float32)
    gain_grad_ref[...] += lax.fori_loop(0, FAR, three_heads, zero)


def qk_backward(core, query, grad_normed, qk_gain):
    tokens, width = query.shape
    block = 128
    return pl.pallas_call(
        qk_kernel,
        grid=(tokens // block,),
        in_specs=[
            pl.BlockSpec(memory_space=pltpu.SMEM),
            pl.BlockSpec((block, width), lambda i: (i, 0)),
            pl.BlockSpec((block, width), lambda i: (i, 0)),
            pl.BlockSpec((1, HEAD), lambda i: (0, 0)),
        ],
        out_specs=[
            pl.BlockSpec((NEAR, FAR, COLS, block), lambda i: (0, 0, 0, i)),
            pl.BlockSpec((NEAR, FAR, COLS, block), lambda i: (0, 0, 0, i)),
            pl.BlockSpec((8, HEAD), lambda i: (0, 0)),
        ],
        out_shape=[
            jax.ShapeDtypeStruct((NEAR, FAR, COLS, tokens), jnp.bfloat16),
            jax.ShapeDtypeStruct((NEAR, FAR, COLS, tokens), jnp.bfloat16),
            jax.ShapeDtypeStruct((8, HEAD), jnp.float32),
        ],
        scratch_shapes=[pltpu.VMEM((block, 3 * HEAD), jnp.bfloat16)],
        compiler_params=pltpu.CompilerParams(dimension_semantics=("arbitrary",)),
        cost_estimate=pl.CostEstimate(
            flops=60_000_000, bytes_accessed=9_500_000, transcendentals=12288
        ),
    )(core, query, grad_normed, qk_gain.reshape(1, HEAD))


def input_kernel(
    near_ref, own_ref, other_ref, query_own_ref, query_other_ref, x_ref, stat_ref, gain_ref,
    slope_ref, sums_ref, gains_ref, grad_ref,
):
    step = pl.program_id(0)

    def product(w_ref, q_ref):
        return lax.dot_general(
            w_ref[...], q_ref[0], (((0,), (0,)), ((), ())), preferred_element_type=jnp.float32
        )

    part = product(own_ref, query_own_ref) + product(other_ref, query_other_ref)

    @pl.when(step == 0)
    def _():
        grad_ref[...] = part

    @pl.when(step > 0)
    def _():
        grad_ref[...] += part

    @pl.when(step == NEAR - 1)
    def _():
        grad = grad_ref[...]
        xhat = (x_ref[...].astype(jnp.float32) - stat_ref[0:1]) * stat_ref[1:2]
        slope = grad * gain_ref[...]
        slope_ref[...] = slope
        sums_ref[0:1] = jnp.sum(slope, axis=0, keepdims=True)
        sums_ref[1:2] = jnp.sum(slope * xhat, axis=0, keepdims=True)
        cross = grad * xhat
        lanes = cross[:, :128] + cross[:, 128:256] + cross[:, 256:384] + cross[:, 384:]
        gains_ref[...] = jnp.sum(jnp.transpose(lanes), axis=0, keepdims=True)


def input_backward(near, own, other, query_own, query_other, x, stat, gain):
    rows, tokens = x.shape
    span = own.shape[0] // NEAR
    whole = lambda i, near: (0, 0)
    return pl.pallas_call(
        input_kernel,
        grid_spec=pltpu.PrefetchScalarGridSpec(
            num_scalar_prefetch=1,
            grid=(NEAR,),
            in_specs=[
                pl.BlockSpec((span, rows), lambda i, near: (i, 0)),
                pl.BlockSpec((span, rows), lambda i, near: (i, 0)),
                pl.BlockSpec((1, span, tokens), lambda i, near: ((near[0] + i) % NEAR, 0, 0)),
                pl.BlockSpec((1, span, tokens), lambda i, near: ((near[0] + i) % NEAR, 0, 0)),
                pl.BlockSpec((rows, tokens), whole),
                pl.BlockSpec((2, tokens), whole),
                pl.BlockSpec((rows, 1), whole),
            ],
            out_specs=[
                pl.BlockSpec((rows, tokens), whole),
                pl.BlockSpec((2, tokens), whole),
                pl.BlockSpec((1, rows), whole),
            ],
            scratch_shapes=[pltpu.VMEM((rows, tokens), jnp.float32)],
        ),
        out_shape=[
            jax.ShapeDtypeStruct((rows, tokens), jnp.float32),
            jax.ShapeDtypeStruct((2, tokens), jnp.float32),
            jax.ShapeDtypeStruct((1, rows), jnp.float32),
        ],
        compiler_params=pltpu.CompilerParams(dimension_semantics=("arbitrary",)),
        cost_estimate=pl.CostEstimate(
            flops=2_400_000_000, bytes_accessed=7_000_000, transcendentals=0
        ),
    )(near, own, other, query_own, query_other, x, stat, gain)


def exchange(x, axes):
    return lax.all_to_all(x, axes, 0, 0, tiled=True)


def shared_by(x, axes):
    copies = jnp.broadcast_to(x[None], (lax.axis_size(axes), *x.shape))
    return exchange(copies, axes)


def summed(x, axes):
    for axis in axes:
        x = jnp.sum(lax.all_gather(x, axis, axis=0), axis=0)
    return x


def swapped(x):
    return lax.ppermute(x, "core", [(0, 1), (1, 0)])


def from_chip(x, distance):
    chips = FAR * NEAR
    return lax.ppermute(x, ("far", "near"), [((i + distance) % chips, i) for i in range(chips)])


def shards(block_input, prenorm_gain, weight, query, grad_normed, qk_gain):
    tokens, rows = block_input.shape
    core = lax.axis_index("core").astype(jnp.int32).reshape(1)
    near = lax.axis_index("near").astype(jnp.int32).reshape(1)

    own = shared_by(weight.T, "far")
    after = from_chip(own, 1)
    before = from_chip(own, -1)
    half = FAR // 2
    across = [from_chip(own[:half], 2), from_chip(own[half:], -2)]
    own = jnp.concatenate([own, after, *across, before]).reshape(-1, rows)
    other = swapped(own)

    x_turned = block_input.T
    x = x_turned.astype(jnp.float32)
    sums = jnp.concatenate([jnp.sum(x, axis=0), jnp.sum(x * x, axis=0)]).reshape(8, 128)
    sums = summed(sums, MP)
    sums = sums.reshape(2, tokens)

    query_own, query_other, qk_partial = qk_backward(core, query, grad_normed, qk_gain)

    mean = sums[0:1] / D
    inv = lax.rsqrt(sums[1:2] / D - mean * mean + EPS)
    xhat = (x - mean) * inv
    gain = prenorm_gain[:, None]
    normed = (xhat * gain).astype(jnp.bfloat16)

    def weight_part(grad_query):
        return lax.dot_general(
            grad_query.reshape(-1, tokens), normed, (((1,), (1,)), ((), ())),
            preferred_element_type=jnp.float32,
        )

    part = weight_part(query_other).astype(jnp.bfloat16)
    from_core = swapped(part)
    part = weight_part(query_own) + from_core.astype(jnp.float32)
    part = part.astype(jnp.bfloat16).reshape(NEAR, FAR, COLS, rows)
    part = exchange(part, "near")
    part = jnp.sum(part.astype(jnp.float32), axis=0).astype(jnp.bfloat16)
    part = exchange(part, "far")
    grad_weight = jnp.sum(part.astype(jnp.float32), axis=0).T

    slope, slopes, gains = input_backward(
        near, own, other, query_own.reshape(NEAR, -1, tokens),
        query_other.reshape(NEAR, -1, tokens), x_turned, jnp.concatenate([mean, inv]), gain,
    )
    slopes = summed(slopes.reshape(8, 128), MP).reshape(2, tokens) / D
    input_gradient = (inv * (slope - slopes[0:1] - xhat * slopes[1:2])).astype(jnp.bfloat16).T

    gains = jnp.concatenate([gains[0], jnp.sum(qk_partial, axis=0)]).reshape(4, 128)
    gains = summed(gains + swapped(gains), ("near", "far")).reshape(-1)
    return (input_gradient, grad_weight, gains[:rows], gains[rows:])


def solution(mesh):
    finer = Mesh(mesh.devices.reshape(FAR, NEAR, 2, 4, 4), (*DP, *MP))
    in_specs = (P(DP, MP), P(MP), P(MP, DP), P(DP, None), P(DP, None), P())
    out_specs = (P(DP, MP), P(MP, DP), P(MP), P())

    return jax.shard_map(
        shards, mesh=finer, in_specs=in_specs, out_specs=out_specs, check_vma=False
    )
```

```python
import jax
import jax.numpy as jnp
from jax import lax
from jax.experimental import pallas as pl
from jax.experimental.pallas import tpu as pltpu
from jax.sharding import Mesh
from jax.sharding import PartitionSpec as P


D = 6144
EPS = 1e-06
HEAD = 128
FAR, NEAR = 8, 4
COLS = 48
MP = ("x", "y")
DP = ("far", "high", "low", "core")


def qk_kernel(
    core_ref, query_ref, grad_ref, gain_ref, own_ref, other_ref, gain_grad_ref, rows_ref
):
    @pl.when(pl.program_id(0) == 0)
    def _():
        gain_grad_ref[...] = jnp.zeros_like(gain_grad_ref)

    core = core_ref[0]
    gain = gain_ref[...]
    scale = 1.0 / HEAD

    def three_heads(group, total):
        for j in range(3):
            cols = pl.ds(pl.multiple_of(group * 384 + j * HEAD, HEAD), HEAD)
            q = query_ref[:, cols].astype(jnp.float32)
            upstream = grad_ref[:, cols].astype(jnp.float32)
            mean = jnp.sum(q, axis=1, keepdims=True) * scale
            var = jnp.sum(q * q, axis=1, keepdims=True) * scale - mean * mean
            inv = lax.rsqrt(var + EPS)
            qhat = (q - mean) * inv
            dqhat = upstream * gain
            mean_d = jnp.sum(dqhat, axis=1, keepdims=True) * scale
            mean_c = jnp.sum(dqhat * qhat, axis=1, keepdims=True) * scale
            rows_ref[:, j * HEAD : (j + 1) * HEAD] = (
                inv * (dqhat - mean_d - qhat * mean_c)
            ).astype(jnp.bfloat16)
            total = total + jnp.sum((upstream * qhat).reshape(-1, 8, HEAD), axis=0)
        turned = jnp.transpose(rows_ref[...])
        for parity, (even_ref, odd_ref) in enumerate(((own_ref, other_ref), (other_ref, own_ref))):

            @pl.when(core == parity)
            def _():
                for b in range(8):
                    to_ref = odd_ref if b % 2 else even_ref
                    to_ref[b // 2, group] = turned[COLS * b : COLS * (b + 1)]

        return total

    zero = jnp.zeros((8, HEAD), jnp.float32)
    gain_grad_ref[...] += lax.fori_loop(0, FAR, three_heads, zero)


def qk_backward(core, query, grad_normed, qk_gain):
    tokens, width = query.shape
    block = 128
    return pl.pallas_call(
        qk_kernel,
        grid=(tokens // block,),
        in_specs=[
            pl.BlockSpec(memory_space=pltpu.SMEM),
            pl.BlockSpec((block, width), lambda i: (i, 0)),
            pl.BlockSpec((block, width), lambda i: (i, 0)),
            pl.BlockSpec((1, HEAD), lambda i: (0, 0)),
        ],
        out_specs=[
            pl.BlockSpec((NEAR, FAR, COLS, block), lambda i: (0, 0, 0, i)),
            pl.BlockSpec((NEAR, FAR, COLS, block), lambda i: (0, 0, 0, i)),
            pl.BlockSpec((8, HEAD), lambda i: (0, 0)),
        ],
        out_shape=[
            jax.ShapeDtypeStruct((NEAR, FAR, COLS, tokens), jnp.bfloat16),
            jax.ShapeDtypeStruct((NEAR, FAR, COLS, tokens), jnp.bfloat16),
            jax.ShapeDtypeStruct((8, HEAD), jnp.float32),
        ],
        scratch_shapes=[pltpu.VMEM((block, 3 * HEAD), jnp.bfloat16)],
        compiler_params=pltpu.CompilerParams(dimension_semantics=("arbitrary",)),
        cost_estimate=pl.CostEstimate(
            flops=60_000_000, bytes_accessed=9_500_000, transcendentals=12288
        ),
    )(core, query, grad_normed, qk_gain.reshape(1, HEAD))


def set_product(core, query_own_ref, query_other_ref):
    def product(w_ref, owner, q_ref):
        w = w_ref[:, owner].reshape(-1, w_ref.shape[-1])
        q = q_ref[0].reshape(-1, q_ref.shape[-1])
        return lax.dot_general(w, q, (((0,), (0,)), ((), ())), preferred_element_type=jnp.float32)

    def both(w_ref):
        return product(w_ref, core, query_own_ref) + product(w_ref, 1 - core, query_other_ref)

    return both


def first_kernel(at_ref, even_ref, odd_ref, query_own_ref, query_other_ref, out_ref):
    both = set_product(at_ref[0], query_own_ref, query_other_ref)

    @pl.when(pl.program_id(0) == 0)
    def _():
        out_ref[...] = both(even_ref)

    @pl.when(pl.program_id(0) == 1)
    def _():
        out_ref[...] += both(odd_ref)


def input_kernel(
    at_ref, even_ref, odd_ref, query_own_ref, query_other_ref, first_ref, x_ref, stat_ref, gain_ref,
    slope_ref, sums_ref, gains_ref, grad_ref,
):
    both = set_product(at_ref[0], query_own_ref, query_other_ref)

    @pl.when(pl.program_id(0) == 0)
    def _():
        grad_ref[...] = first_ref[...] + both(even_ref)

    @pl.when(pl.program_id(0) == 1)
    def _():
        grad = grad_ref[...] + both(odd_ref)
        xhat = (x_ref[...].astype(jnp.float32) - stat_ref[0:1]) * stat_ref[1:2]
        slope = grad * gain_ref[...]
        slope_ref[...] = slope
        sums_ref[0:1] = jnp.sum(slope, axis=0, keepdims=True)
        sums_ref[1:2] = jnp.sum(slope * xhat, axis=0, keepdims=True)
        cross = grad * xhat
        lanes = cross[:, :128] + cross[:, 128:256] + cross[:, 256:384] + cross[:, 384:]
        gains_ref[...] = jnp.sum(jnp.transpose(lanes), axis=0, keepdims=True)


def input_part(body, at, even, odd, query_own, query_other, extra, outs, scratch):
    tokens = query_own.shape[-1]
    span = query_own.shape[1:]

    def whole(shape):
        return pl.BlockSpec(shape, lambda i, at: (0,) * len(shape))

    query_spec = pl.BlockSpec((1, *span), lambda i, at: (2 * i + at[1], 0, 0, 0))
    return pl.pallas_call(
        body,
        grid_spec=pltpu.PrefetchScalarGridSpec(
            num_scalar_prefetch=1,
            grid=(2,),
            in_specs=[whole(even.shape), whole(odd.shape), query_spec, query_spec]
            + [whole(e.shape) for e in extra],
            out_specs=[whole(o) for o in outs],
            scratch_shapes=scratch,
        ),
        out_shape=[jax.ShapeDtypeStruct(o, jnp.float32) for o in outs],
        compiler_params=pltpu.CompilerParams(dimension_semantics=("arbitrary",)),
        cost_estimate=pl.CostEstimate(
            flops=2 * 1536 * 384 * tokens, bytes_accessed=4_500_000, transcendentals=0
        ),
    )(at, even, odd, query_own, query_other, *extra)


def exchange(x, axes):
    return lax.all_to_all(x, axes, 0, 0, tiled=True)


def shared_by(x, axes):
    copies = jnp.broadcast_to(x[None], (lax.axis_size(axes), *x.shape))
    return exchange(copies, axes)


def summed(x, axes):
    for axis in axes:
        x = jnp.sum(lax.all_gather(x, axis, axis=0), axis=0)
    return x


def swapped(x):
    return lax.ppermute(x, "core", [(0, 1), (1, 0)])


def from_chip(x, distance):
    chips = FAR * NEAR
    return lax.ppermute(x, ("far", "high", "low"), [((i + distance) % chips, i) for i in range(chips)])


def shards(block_input, prenorm_gain, weight, query, grad_normed, qk_gain):
    tokens, rows = block_input.shape
    core = lax.axis_index("core").astype(jnp.int32)
    parity = lax.axis_index("low").astype(jnp.int32)

    mine = lax.all_gather(weight.T, ("far", "high", "core"), axis=0)
    mine = mine.reshape(FAR, 2, 2, COLS, rows)
    even, odd = mine[:, 0], mine[:, 1]
    theirs_even = from_chip(even, 1)
    theirs_odd = from_chip(odd, -1)

    x_turned = block_input.T
    x = x_turned.astype(jnp.float32)
    sums = jnp.concatenate([jnp.sum(x, axis=0), jnp.sum(x * x, axis=0)]).reshape(8, 128)
    sums = shared_by(sums, MP)
    sums = jnp.sum(sums, axis=0).reshape(2, tokens)

    query_own, query_other, qk_partial = qk_backward(core.reshape(1), query, grad_normed, qk_gain)

    mean = sums[0:1] / D
    inv = lax.rsqrt(sums[1:2] / D - mean * mean + EPS)
    xhat = (x - mean) * inv
    gain = prenorm_gain[:, None]
    normed = (xhat * gain).astype(jnp.bfloat16)

    def weight_part(grad_query):
        return lax.dot_general(
            grad_query.reshape(-1, tokens), normed, (((1,), (1,)), ((), ())),
            preferred_element_type=jnp.float32,
        )

    part = weight_part(query_other).astype(jnp.bfloat16)
    from_core = swapped(part)
    part = weight_part(query_own) + from_core.astype(jnp.float32)
    part = part.astype(jnp.bfloat16).reshape(NEAR, FAR, COLS, rows)
    part = exchange(part, ("high", "low"))
    part = jnp.sum(part.astype(jnp.float32), axis=0).astype(jnp.bfloat16)
    part = exchange(part, "far")
    grad_weight = jnp.sum(part.astype(jnp.float32), axis=0).T

    (first,) = input_part(
        first_kernel, jnp.stack([core, parity]), even, odd, query_own, query_other,
        (), ((rows, tokens),), (),
    )
    slope, slopes, gains = input_part(
        input_kernel, jnp.stack([core, 1 - parity]), theirs_even, theirs_odd,
        query_own, query_other, (first, x_turned, jnp.concatenate([mean, inv]), gain),
        ((rows, tokens), (2, tokens), (1, rows)), (pltpu.VMEM((rows, tokens), jnp.float32),),
    )
    slopes = summed(slopes.reshape(8, 128), MP).reshape(2, tokens) / D
    input_gradient = (inv * (slope - slopes[0:1] - xhat * slopes[1:2])).astype(jnp.bfloat16).T

    gains = jnp.concatenate([gains[0], jnp.sum(qk_partial, axis=0)]).reshape(4, 128)
    gains = gains + swapped(gains)
    gains = shared_by(gains, ("far", "high", "low"))
    gains = jnp.sum(gains, axis=0).reshape(-1)
    return (input_gradient, grad_weight, gains[:rows], gains[rows:])


def solution(mesh):
    finer = Mesh(mesh.devices.reshape(FAR, 2, 2, 2, 4, 4), (*DP, *MP))
    in_specs = (P(DP, MP), P(MP), P(MP, DP), P(DP, None), P(DP, None), P())
    out_specs = (P(DP, MP), P(MP, DP), P(MP), P())

    return jax.shard_map(
        shards, mesh=finer, in_specs=in_specs, out_specs=out_specs, check_vma=False
    )
```

```python
import jax
import jax.numpy as jnp
from jax import lax
from jax.experimental import pallas as pl
from jax.experimental.pallas import tpu as pltpu
from jax.sharding import Mesh
from jax.sharding import PartitionSpec as P


D = 6144
EPS = 1e-06
HEAD = 128
FAR, NEAR = 8, 4
COLS = 48
MP = ("x", "y")
DP = ("far", "high", "low", "core")


def qk_kernel(
    core_ref, query_ref, grad_ref, gain_ref, own_ref, other_ref, gain_grad_ref, rows_ref
):
    @pl.when(pl.program_id(0) == 0)
    def _():
        gain_grad_ref[...] = jnp.zeros_like(gain_grad_ref)

    core = core_ref[0]
    gain = gain_ref[...]
    scale = 1.0 / HEAD

    def three_heads(group, total):
        for j in range(3):
            cols = pl.ds(pl.multiple_of(group * 384 + j * HEAD, HEAD), HEAD)
            q = query_ref[:, cols].astype(jnp.float32)
            upstream = grad_ref[:, cols].astype(jnp.float32)
            mean = jnp.sum(q, axis=1, keepdims=True) * scale
            var = jnp.sum(q * q, axis=1, keepdims=True) * scale - mean * mean
            inv = lax.rsqrt(var + EPS)
            qhat = (q - mean) * inv
            dqhat = upstream * gain
            mean_d = jnp.sum(dqhat, axis=1, keepdims=True) * scale
            mean_c = jnp.sum(dqhat * qhat, axis=1, keepdims=True) * scale
            rows_ref[:, j * HEAD : (j + 1) * HEAD] = (
                inv * (dqhat - mean_d - qhat * mean_c)
            ).astype(jnp.bfloat16)
            total = total + jnp.sum((upstream * qhat).reshape(-1, 8, HEAD), axis=0)
        turned = jnp.transpose(rows_ref[...])
        for parity, (even_ref, odd_ref) in enumerate(((own_ref, other_ref), (other_ref, own_ref))):

            @pl.when(core == parity)
            def _():
                for b in range(8):
                    to_ref = odd_ref if b % 2 else even_ref
                    to_ref[b // 2, group] = turned[COLS * b : COLS * (b + 1)]

        return total

    zero = jnp.zeros((8, HEAD), jnp.float32)
    gain_grad_ref[...] += lax.fori_loop(0, FAR, three_heads, zero)


def qk_backward(core, query, grad_normed, qk_gain):
    tokens, width = query.shape
    block = 128
    return pl.pallas_call(
        qk_kernel,
        grid=(tokens // block,),
        in_specs=[
            pl.BlockSpec(memory_space=pltpu.SMEM),
            pl.BlockSpec((block, width), lambda i: (i, 0)),
            pl.BlockSpec((block, width), lambda i: (i, 0)),
            pl.BlockSpec((1, HEAD), lambda i: (0, 0)),
        ],
        out_specs=[
            pl.BlockSpec((NEAR, FAR, COLS, block), lambda i: (0, 0, 0, i)),
            pl.BlockSpec((NEAR, FAR, COLS, block), lambda i: (0, 0, 0, i)),
            pl.BlockSpec((8, HEAD), lambda i: (0, 0)),
        ],
        out_shape=[
            jax.ShapeDtypeStruct((NEAR, FAR, COLS, tokens), jnp.bfloat16),
            jax.ShapeDtypeStruct((NEAR, FAR, COLS, tokens), jnp.bfloat16),
            jax.ShapeDtypeStruct((8, HEAD), jnp.float32),
        ],
        scratch_shapes=[pltpu.VMEM((block, 3 * HEAD), jnp.bfloat16)],
        compiler_params=pltpu.CompilerParams(dimension_semantics=("arbitrary",)),
        cost_estimate=pl.CostEstimate(
            flops=60_000_000, bytes_accessed=9_500_000, transcendentals=12288
        ),
    )(core, query, grad_normed, qk_gain.reshape(1, HEAD))


def input_kernel(
    core_ref, w_ref, query_own_ref, query_other_ref, x_ref, stat_ref, gain_ref,
    slope_ref, sums_ref, gains_ref, grad_ref,
):
    core = core_ref[0]
    step = pl.program_id(0)

    def product(owner, q_ref):
        w = w_ref[:, 0, owner].reshape(-1, w_ref.shape[-1])
        q = q_ref[0].reshape(-1, q_ref.shape[-1])
        return lax.dot_general(w, q, (((0,), (0,)), ((), ())), preferred_element_type=jnp.float32)

    part = product(core, query_own_ref) + product(1 - core, query_other_ref)

    @pl.when(step == 0)
    def _():
        grad_ref[...] = part

    @pl.when(step > 0)
    def _():
        grad_ref[...] += part

    @pl.when(step == NEAR - 1)
    def _():
        grad = grad_ref[...]
        xhat = (x_ref[...].astype(jnp.float32) - stat_ref[0:1]) * stat_ref[1:2]
        slope = grad * gain_ref[...]
        slope_ref[...] = slope
        sums_ref[0:1] = jnp.sum(slope, axis=0, keepdims=True)
        sums_ref[1:2] = jnp.sum(slope * xhat, axis=0, keepdims=True)
        cross = grad * xhat
        lanes = cross[:, :128] + cross[:, 128:256] + cross[:, 256:384] + cross[:, 384:]
        gains_ref[...] = jnp.sum(jnp.transpose(lanes), axis=0, keepdims=True)


def input_backward(core, columns, query_own, query_other, x, stat, gain):
    rows, tokens = x.shape

    def whole(shape):
        return pl.BlockSpec(shape, lambda i, core: (0,) * len(shape))

    query_spec = pl.BlockSpec((1, *query_own.shape[1:]), lambda i, core: (i, 0, 0, 0))
    outs = ((rows, tokens), (2, tokens), (1, rows))
    return pl.pallas_call(
        input_kernel,
        grid_spec=pltpu.PrefetchScalarGridSpec(
            num_scalar_prefetch=1,
            grid=(NEAR,),
            in_specs=[
                pl.BlockSpec((FAR, 1, 2, COLS, rows), lambda i, core: (0, i, 0, 0, 0)),
                query_spec,
                query_spec,
                whole(x.shape),
                whole(stat.shape),
                whole(gain.shape),
            ],
            out_specs=[whole(o) for o in outs],
            scratch_shapes=[pltpu.VMEM((rows, tokens), jnp.float32)],
        ),
        out_shape=[jax.ShapeDtypeStruct(o, jnp.float32) for o in outs],
        compiler_params=pltpu.CompilerParams(dimension_semantics=("arbitrary",)),
        cost_estimate=pl.CostEstimate(
            flops=2 * 3072 * rows * tokens, bytes_accessed=7_000_000, transcendentals=0
        ),
    )(core, columns, query_own, query_other, x, stat, gain)


def exchange(x, axes):
    return lax.all_to_all(x, axes, 0, 0, tiled=True)


def shared_by(x, axes):
    copies = jnp.broadcast_to(x[None], (lax.axis_size(axes), *x.shape))
    return exchange(copies, axes)


def summed(x, axes):
    for axis in axes:
        x = jnp.sum(lax.all_gather(x, axis, axis=0), axis=0)
    return x


def swapped(x):
    return lax.ppermute(x, "core", [(0, 1), (1, 0)])


def shards(block_input, prenorm_gain, weight, query, grad_normed, qk_gain):
    tokens, rows = block_input.shape
    core = lax.axis_index("core").astype(jnp.int32).reshape(1)

    columns = lax.all_gather(weight.T, DP, axis=0).reshape(FAR, NEAR, 2, COLS, rows)

    x_turned = block_input.T
    x = x_turned.astype(jnp.float32)
    sums = jnp.concatenate([jnp.sum(x, axis=0), jnp.sum(x * x, axis=0)]).reshape(8, 128)
    sums = shared_by(sums, MP)
    sums = jnp.sum(sums, axis=0).reshape(2, tokens)

    query_own, query_other, qk_partial = qk_backward(core, query, grad_normed, qk_gain)

    mean = sums[0:1] / D
    inv = lax.rsqrt(sums[1:2] / D - mean * mean + EPS)
    xhat = (x - mean) * inv
    gain = prenorm_gain[:, None]
    normed = (xhat * gain).astype(jnp.bfloat16)

    def weight_part(grad_query):
        return lax.dot_general(
            grad_query.reshape(-1, tokens), normed, (((1,), (1,)), ((), ())),
            preferred_element_type=jnp.float32,
        )

    part = weight_part(query_other).astype(jnp.bfloat16)
    from_core = swapped(part)
    part = weight_part(query_own) + from_core.astype(jnp.float32)
    part = part.astype(jnp.bfloat16).reshape(NEAR, FAR, COLS, rows)
    part = exchange(part, ("high", "low"))
    part = jnp.sum(part.astype(jnp.float32), axis=0).astype(jnp.bfloat16)
    part = exchange(part, "far")
    grad_weight = jnp.sum(part.astype(jnp.float32), axis=0).T

    slope, slopes, gains = input_backward(
        core, columns, query_own, query_other, x_turned, jnp.concatenate([mean, inv]), gain
    )
    slopes = summed(slopes.reshape(8, 128), MP).reshape(2, tokens) / D
    input_gradient = (inv * (slope - slopes[0:1] - xhat * slopes[1:2])).astype(jnp.bfloat16).T

    gains = jnp.concatenate([gains[0], jnp.sum(qk_partial, axis=0)]).reshape(4, 128)
    gains = gains + swapped(gains)
    gains = shared_by(gains, ("far", "high", "low"))
    gains = jnp.sum(gains, axis=0).reshape(-1)
    return (input_gradient, grad_weight, gains[:rows], gains[rows:])


def solution(mesh):
    finer = Mesh(mesh.devices.reshape(FAR, 2, 2, 2, 4, 4), (*DP, *MP))
    in_specs = (P(DP, MP), P(MP), P(MP, DP), P(DP, None), P(DP, None), P())
    out_specs = (P(DP, MP), P(MP, DP), P(MP), P())

    return jax.shard_map(
        shards, mesh=finer, in_specs=in_specs, out_specs=out_specs, check_vma=False
    )
```

```python
import jax
import jax.numpy as jnp
from jax import lax
from jax.experimental import pallas as pl
from jax.experimental.pallas import tpu as pltpu
from jax.sharding import Mesh
from jax.sharding import PartitionSpec as P


D = 6144
EPS = 1e-06
HEAD = 128
FAR, NEAR = 8, 4
COLS = 48
MP = ("x", "y")
DP = ("far", "high", "low", "core")


def qk_kernel(
    core_ref, query_ref, grad_ref, gain_ref, own_ref, other_ref, gain_grad_ref, rows_ref
):
    @pl.when(pl.program_id(0) == 0)
    def _():
        gain_grad_ref[...] = jnp.zeros_like(gain_grad_ref)

    core = core_ref[0]
    gain = gain_ref[...]
    scale = 1.0 / HEAD

    def three_heads(group, total):
        for j in range(3):
            cols = pl.ds(pl.multiple_of(group * 384 + j * HEAD, HEAD), HEAD)
            q = query_ref[:, cols].astype(jnp.float32)
            upstream = grad_ref[:, cols].astype(jnp.float32)
            mean = jnp.sum(q, axis=1, keepdims=True) * scale
            var = jnp.sum(q * q, axis=1, keepdims=True) * scale - mean * mean
            inv = lax.rsqrt(var + EPS)
            qhat = (q - mean) * inv
            dqhat = upstream * gain
            mean_d = jnp.sum(dqhat, axis=1, keepdims=True) * scale
            mean_c = jnp.sum(dqhat * qhat, axis=1, keepdims=True) * scale
            rows_ref[:, j * HEAD : (j + 1) * HEAD] = (
                inv * (dqhat - mean_d - qhat * mean_c)
            ).astype(jnp.bfloat16)
            total = total + jnp.sum((upstream * qhat).reshape(-1, 8, HEAD), axis=0)
        turned = jnp.transpose(rows_ref[...])
        for parity, (even_ref, odd_ref) in enumerate(((own_ref, other_ref), (other_ref, own_ref))):

            @pl.when(core == parity)
            def _():
                for b in range(8):
                    to_ref = odd_ref if b % 2 else even_ref
                    to_ref[b // 2, group] = turned[COLS * b : COLS * (b + 1)]

        return total

    zero = jnp.zeros((8, HEAD), jnp.float32)
    gain_grad_ref[...] += lax.fori_loop(0, FAR, three_heads, zero)


def qk_backward(core, query, grad_normed, qk_gain):
    tokens, width = query.shape
    block = 128
    return pl.pallas_call(
        qk_kernel,
        grid=(tokens // block,),
        in_specs=[
            pl.BlockSpec(memory_space=pltpu.SMEM),
            pl.BlockSpec((block, width), lambda i: (i, 0)),
            pl.BlockSpec((block, width), lambda i: (i, 0)),
            pl.BlockSpec((1, HEAD), lambda i: (0, 0)),
        ],
        out_specs=[
            pl.BlockSpec((NEAR, FAR, COLS, block), lambda i: (0, 0, 0, i)),
            pl.BlockSpec((NEAR, FAR, COLS, block), lambda i: (0, 0, 0, i)),
            pl.BlockSpec((8, HEAD), lambda i: (0, 0)),
        ],
        out_shape=[
            jax.ShapeDtypeStruct((NEAR, FAR, COLS, tokens), jnp.bfloat16),
            jax.ShapeDtypeStruct((NEAR, FAR, COLS, tokens), jnp.bfloat16),
            jax.ShapeDtypeStruct((8, HEAD), jnp.float32),
        ],
        scratch_shapes=[pltpu.VMEM((block, 3 * HEAD), jnp.bfloat16)],
        compiler_params=pltpu.CompilerParams(dimension_semantics=("arbitrary",)),
        cost_estimate=pl.CostEstimate(
            flops=60_000_000, bytes_accessed=9_500_000, transcendentals=12288
        ),
    )(core, query, grad_normed, qk_gain.reshape(1, HEAD))


def set_product(query_own_ref, query_other_ref):
    def product(w_ref, owner, q_ref):
        w = w_ref[:, owner].reshape(-1, w_ref.shape[-1])
        q = q_ref[0].reshape(-1, q_ref.shape[-1])
        return lax.dot_general(w, q, (((0,), (0,)), ((), ())), preferred_element_type=jnp.float32)

    def both(w_ref):
        return product(w_ref, 0, query_own_ref) + product(w_ref, 1, query_other_ref)

    return both


def first_kernel(at_ref, even_ref, odd_ref, query_own_ref, query_other_ref, out_ref):
    both = set_product(query_own_ref, query_other_ref)

    @pl.when(pl.program_id(0) == 0)
    def _():
        out_ref[...] = both(even_ref)

    @pl.when(pl.program_id(0) == 1)
    def _():
        out_ref[...] += both(odd_ref)


def input_kernel(
    at_ref, even_ref, odd_ref, query_own_ref, query_other_ref, first_ref, x_ref, stat_ref, gain_ref,
    slope_ref, sums_ref, gains_ref, grad_ref,
):
    both = set_product(query_own_ref, query_other_ref)

    @pl.when(pl.program_id(0) == 0)
    def _():
        grad_ref[...] = first_ref[...] + both(even_ref)

    @pl.when(pl.program_id(0) == 1)
    def _():
        grad = grad_ref[...] + both(odd_ref)
        xhat = (x_ref[...].astype(jnp.float32) - stat_ref[0:1]) * stat_ref[1:2]
        slope = grad * gain_ref[...]
        slope_ref[...] = slope
        sums_ref[0:1] = jnp.sum(slope, axis=0, keepdims=True)
        sums_ref[1:2] = jnp.sum(slope * xhat, axis=0, keepdims=True)
        cross = grad * xhat
        lanes = cross[:, :128] + cross[:, 128:256] + cross[:, 256:384] + cross[:, 384:]
        gains_ref[...] = jnp.sum(jnp.transpose(lanes), axis=0, keepdims=True)


def input_part(body, at, even, odd, query_own, query_other, extra, outs, scratch):
    tokens = query_own.shape[-1]
    span = query_own.shape[1:]

    def whole(shape):
        return pl.BlockSpec(shape, lambda i, at: (0,) * len(shape))

    query_spec = pl.BlockSpec((1, *span), lambda i, at: (2 * i + at[0], 0, 0, 0))
    return pl.pallas_call(
        body,
        grid_spec=pltpu.PrefetchScalarGridSpec(
            num_scalar_prefetch=1,
            grid=(2,),
            in_specs=[whole(even.shape), whole(odd.shape), query_spec, query_spec]
            + [whole(e.shape) for e in extra],
            out_specs=[whole(o) for o in outs],
            scratch_shapes=scratch,
        ),
        out_shape=[jax.ShapeDtypeStruct(o, jnp.float32) for o in outs],
        compiler_params=pltpu.CompilerParams(dimension_semantics=("arbitrary",)),
        cost_estimate=pl.CostEstimate(
            flops=2 * 1536 * 384 * tokens, bytes_accessed=4_500_000, transcendentals=0
        ),
    )(at, even, odd, query_own, query_other, *extra)


def exchange(x, axes):
    return lax.all_to_all(x, axes, 0, 0, tiled=True)


def shared_by(x, axes):
    copies = jnp.broadcast_to(x[None], (lax.axis_size(axes), *x.shape))
    return exchange(copies, axes)


def thirds(x):
    high = lax.reduce_precision(x, 8, 7)
    middle = lax.reduce_precision(x - high, 8, 7)
    return jnp.stack([high, middle, x - high - middle]).astype(jnp.bfloat16)


def summed(x, axes):
    for axis in axes:
        x = jnp.sum(lax.all_gather(x, axis, axis=0), axis=0)
    return x


def swapped(x):
    return lax.ppermute(x, "core", [(0, 1), (1, 0)])


def from_chip(x, distance):
    chips = FAR * NEAR
    return lax.ppermute(x, ("far", "high", "low"), [((i + distance) % chips, i) for i in range(chips)])


def shards(block_input, prenorm_gain, weight, query, grad_normed, qk_gain):
    tokens, rows = block_input.shape
    core = lax.axis_index("core").astype(jnp.int32)
    parity = lax.axis_index("low").astype(jnp.int32).reshape(1)

    mine = weight.T
    mine = jnp.stack([mine, swapped(mine)])
    mine = lax.all_gather(mine, ("far", "high"), axis=0).reshape(FAR, 2, 2, COLS, rows)
    even, odd = mine[:, 0], mine[:, 1]
    theirs_even = from_chip(even, 1)
    theirs_odd = from_chip(odd, -1)

    x_turned = block_input.T
    x = x_turned.astype(jnp.float32)
    sums = jnp.concatenate([jnp.sum(x, axis=0), jnp.sum(x * x, axis=0)]).reshape(8, 128)
    sums = shared_by(sums, MP)
    sums = jnp.sum(sums, axis=0).reshape(2, tokens)

    query_own, query_other, qk_partial = qk_backward(core.reshape(1), query, grad_normed, qk_gain)

    mean = sums[0:1] / D
    inv = lax.rsqrt(sums[1:2] / D - mean * mean + EPS)
    xhat = (x - mean) * inv
    gain = prenorm_gain[:, None]
    normed = (xhat * gain).astype(jnp.bfloat16)

    def weight_part(grad_query):
        return lax.dot_general(
            grad_query.reshape(-1, tokens), normed, (((1,), (1,)), ((), ())),
            preferred_element_type=jnp.float32,
        )

    part = weight_part(query_other).astype(jnp.bfloat16)
    from_core = swapped(part)
    part = weight_part(query_own) + from_core.astype(jnp.float32)
    part = part.astype(jnp.bfloat16).reshape(NEAR, FAR, COLS, rows)
    part = exchange(part, ("high", "low"))
    part = jnp.sum(part.astype(jnp.float32), axis=0).astype(jnp.bfloat16)

    (first,) = input_part(
        first_kernel, parity, even, odd, query_own, query_other,
        (), ((rows, tokens),), (),
    )
    slope, slopes, gains = input_part(
        input_kernel, 1 - parity, theirs_even, theirs_odd,
        query_own, query_other, (first, x_turned, jnp.concatenate([mean, inv]), gain),
        ((rows, tokens), (2, tokens), (1, rows)), (pltpu.VMEM((rows, tokens), jnp.float32),),
    )
    slopes = summed(slopes.reshape(8, 128), MP).reshape(2, tokens) / D
    input_gradient = (inv * (slope - slopes[0:1] - xhat * slopes[1:2])).astype(jnp.bfloat16).T

    gains = jnp.concatenate([gains[0], jnp.sum(qk_partial, axis=0)])
    gains = gains + swapped(gains.reshape(4, 128)).reshape(-1)
    rest = jnp.pad(thirds(gains).reshape(-1, rows), ((0, 4), (0, 0)))
    part = jnp.concatenate([part, jnp.broadcast_to(rest[None], (FAR, *rest.shape))], axis=1)
    part = exchange(part, "far")
    part = jnp.sum(part.astype(jnp.float32), axis=0)
    grad_weight = part[:COLS].T
    gains = jnp.sum(part[COLS : COLS + 4].reshape(3, 4, 128), axis=0)
    gains = jnp.sum(lax.all_gather(gains, ("high", "low"), axis=0), axis=0).reshape(-1)
    return (input_gradient, grad_weight, gains[:rows], gains[rows:])


def solution(mesh):
    finer = Mesh(mesh.devices.reshape(FAR, 2, 2, 2, 4, 4), (*DP, *MP))
    in_specs = (P(DP, MP), P(MP), P(MP, DP), P(DP, None), P(DP, None), P())
    out_specs = (P(DP, MP), P(MP, DP), P(MP), P())

    return jax.shard_map(
        shards, mesh=finer, in_specs=in_specs, out_specs=out_specs, check_vma=False
    )
```

```python
import jax
import jax.numpy as jnp
from jax import lax
from jax.experimental import pallas as pl
from jax.experimental.pallas import tpu as pltpu
from jax.sharding import Mesh
from jax.sharding import PartitionSpec as P


D = 6144
EPS = 1e-06
HEAD = 128
FAR, NEAR = 8, 4
COLS = 48
MP = ("x", "y")
DP = ("far", "high", "low", "core")


def qk_kernel(
    core_ref, query_ref, grad_ref, gain_ref, own_ref, other_ref, gain_grad_ref, rows_ref
):
    @pl.when(pl.program_id(0) == 0)
    def _():
        gain_grad_ref[...] = jnp.zeros_like(gain_grad_ref)

    core = core_ref[0]
    gain = gain_ref[...]
    scale = 1.0 / HEAD

    def three_heads(group, total):
        for j in range(3):
            cols = pl.ds(pl.multiple_of(group * 384 + j * HEAD, HEAD), HEAD)
            q = query_ref[:, cols].astype(jnp.float32)
            upstream = grad_ref[:, cols].astype(jnp.float32)
            mean = jnp.sum(q, axis=1, keepdims=True) * scale
            var = jnp.sum(q * q, axis=1, keepdims=True) * scale - mean * mean
            inv = lax.rsqrt(var + EPS)
            qhat = (q - mean) * inv
            dqhat = upstream * gain
            mean_d = jnp.sum(dqhat, axis=1, keepdims=True) * scale
            mean_c = jnp.sum(dqhat * qhat, axis=1, keepdims=True) * scale
            rows_ref[:, j * HEAD : (j + 1) * HEAD] = (
                inv * (dqhat - mean_d - qhat * mean_c)
            ).astype(jnp.bfloat16)
            total = total + jnp.sum((upstream * qhat).reshape(-1, 8, HEAD), axis=0)
        turned = jnp.transpose(rows_ref[...])
        for parity, (even_ref, odd_ref) in enumerate(((own_ref, other_ref), (other_ref, own_ref))):

            @pl.when(core == parity)
            def _():
                for b in range(8):
                    to_ref = odd_ref if b % 2 else even_ref
                    to_ref[b // 2, group] = turned[COLS * b : COLS * (b + 1)]

        return total

    zero = jnp.zeros((8, HEAD), jnp.float32)
    gain_grad_ref[...] += lax.fori_loop(0, FAR, three_heads, zero)


def qk_backward(core, query, grad_normed, qk_gain):
    tokens, width = query.shape
    block = 128
    return pl.pallas_call(
        qk_kernel,
        grid=(tokens // block,),
        in_specs=[
            pl.BlockSpec(memory_space=pltpu.SMEM),
            pl.BlockSpec((block, width), lambda i: (i, 0)),
            pl.BlockSpec((block, width), lambda i: (i, 0)),
            pl.BlockSpec((1, HEAD), lambda i: (0, 0)),
        ],
        out_specs=[
            pl.BlockSpec((NEAR, FAR, COLS, block), lambda i: (0, 0, 0, i)),
            pl.BlockSpec((NEAR, FAR, COLS, block), lambda i: (0, 0, 0, i)),
            pl.BlockSpec((8, HEAD), lambda i: (0, 0)),
        ],
        out_shape=[
            jax.ShapeDtypeStruct((NEAR, FAR, COLS, tokens), jnp.bfloat16),
            jax.ShapeDtypeStruct((NEAR, FAR, COLS, tokens), jnp.bfloat16),
            jax.ShapeDtypeStruct((8, HEAD), jnp.float32),
        ],
        scratch_shapes=[pltpu.VMEM((block, 3 * HEAD), jnp.bfloat16)],
        compiler_params=pltpu.CompilerParams(dimension_semantics=("arbitrary",)),
        cost_estimate=pl.CostEstimate(
            flops=60_000_000, bytes_accessed=9_500_000, transcendentals=12288
        ),
    )(core, query, grad_normed, qk_gain.reshape(1, HEAD))


def input_kernel(
    at_ref, own_ref, other_ref, query_own_ref, query_other_ref, x_ref, stat_ref, gain_ref,
    slope_ref, sums_ref, gains_ref, grad_ref,
):
    step = pl.program_id(0)

    def product(w_ref, q_ref):
        return lax.dot_general(
            w_ref[...], q_ref[0], (((0,), (0,)), ((), ())), preferred_element_type=jnp.float32
        )

    part = product(own_ref, query_own_ref) + product(other_ref, query_other_ref)

    @pl.when(step == 0)
    def _():
        grad_ref[...] = part

    @pl.when(step > 0)
    def _():
        grad_ref[...] += part

    @pl.when(step == NEAR - 1)
    def _():
        grad = grad_ref[...]
        xhat = (x_ref[...].astype(jnp.float32) - stat_ref[0:1]) * stat_ref[1:2]
        slope = grad * gain_ref[...]
        slope_ref[...] = slope
        sums_ref[0:1] = jnp.sum(slope, axis=0, keepdims=True)
        sums_ref[1:2] = jnp.sum(slope * xhat, axis=0, keepdims=True)
        cross = grad * xhat
        lanes = cross[:, :128] + cross[:, 128:256] + cross[:, 256:384] + cross[:, 384:]
        gains_ref[...] = jnp.sum(jnp.transpose(lanes), axis=0, keepdims=True)


def input_backward(at, own, other, query_own, query_other, x, stat, gain):
    rows, tokens = x.shape
    span = own.shape[0] // NEAR
    whole = lambda i, at: (0, 0)
    return pl.pallas_call(
        input_kernel,
        grid_spec=pltpu.PrefetchScalarGridSpec(
            num_scalar_prefetch=1,
            grid=(NEAR,),
            in_specs=[
                pl.BlockSpec((span, rows), lambda i, at: (i, 0)),
                pl.BlockSpec((span, rows), lambda i, at: (i, 0)),
                pl.BlockSpec((1, span, tokens), lambda i, at: (2 * (i % 2) + (at[0] + i // 2) % 2, 0, 0)),
                pl.BlockSpec((1, span, tokens), lambda i, at: (2 * (i % 2) + (at[0] + i // 2) % 2, 0, 0)),
                pl.BlockSpec((rows, tokens), whole),
                pl.BlockSpec((2, tokens), whole),
                pl.BlockSpec((rows, 1), whole),
            ],
            out_specs=[
                pl.BlockSpec((rows, tokens), whole),
                pl.BlockSpec((2, tokens), whole),
                pl.BlockSpec((1, rows), whole),
            ],
            scratch_shapes=[pltpu.VMEM((rows, tokens), jnp.float32)],
        ),
        out_shape=[
            jax.ShapeDtypeStruct((rows, tokens), jnp.float32),
            jax.ShapeDtypeStruct((2, tokens), jnp.float32),
            jax.ShapeDtypeStruct((1, rows), jnp.float32),
        ],
        compiler_params=pltpu.CompilerParams(dimension_semantics=("arbitrary",)),
        cost_estimate=pl.CostEstimate(
            flops=2_400_000_000, bytes_accessed=7_000_000, transcendentals=0
        ),
    )(at, own, other, query_own, query_other, x, stat, gain)


def exchange(x, axes):
    return lax.all_to_all(x, axes, 0, 0, tiled=True)


def shared_by(x, axes):
    copies = jnp.broadcast_to(x[None], (lax.axis_size(axes), *x.shape))
    return exchange(copies, axes)


def thirds(x):
    high = lax.reduce_precision(x, 8, 7)
    middle = lax.reduce_precision(x - high, 8, 7)
    return jnp.stack([high, middle, x - high - middle]).astype(jnp.bfloat16)


def summed(x, axes):
    for axis in axes:
        x = jnp.sum(lax.all_gather(x, axis, axis=0), axis=0)
    return x


def swapped(x):
    return lax.ppermute(x, "core", [(0, 1), (1, 0)])


def from_chip(x, distance):
    chips = FAR * NEAR
    return lax.ppermute(x, ("far", "high", "low"), [((i + distance) % chips, i) for i in range(chips)])


def shards(block_input, prenorm_gain, weight, query, grad_normed, qk_gain):
    tokens, rows = block_input.shape
    core = lax.axis_index("core").astype(jnp.int32)
    parity = lax.axis_index("low").astype(jnp.int32).reshape(1)

    own = lax.all_gather(weight.T, ("far", "high"), axis=0).reshape(FAR, 2, COLS, rows)
    even, odd = own[:, 0], own[:, 1]
    theirs_even = from_chip(even, 1)
    theirs_odd = from_chip(odd, -1)
    own = jnp.concatenate([even, odd, theirs_even, theirs_odd]).reshape(-1, rows)
    other = swapped(own)

    x_turned = block_input.T
    x = x_turned.astype(jnp.float32)
    sums = jnp.concatenate([jnp.sum(x, axis=0), jnp.sum(x * x, axis=0)]).reshape(8, 128)
    sums = shared_by(sums, MP)
    sums = jnp.sum(sums, axis=0).reshape(2, tokens)

    query_own, query_other, qk_partial = qk_backward(core.reshape(1), query, grad_normed, qk_gain)

    mean = sums[0:1] / D
    inv = lax.rsqrt(sums[1:2] / D - mean * mean + EPS)
    xhat = (x - mean) * inv
    gain = prenorm_gain[:, None]
    normed = (xhat * gain).astype(jnp.bfloat16)

    def weight_part(grad_query):
        return lax.dot_general(
            grad_query.reshape(-1, tokens), normed, (((1,), (1,)), ((), ())),
            preferred_element_type=jnp.float32,
        )

    part = weight_part(query_other).astype(jnp.bfloat16)
    from_core = swapped(part)
    part = weight_part(query_own) + from_core.astype(jnp.float32)
    part = part.astype(jnp.bfloat16).reshape(NEAR, FAR, COLS, rows)
    part = exchange(part, ("high", "low"))
    part = jnp.sum(part.astype(jnp.float32), axis=0).astype(jnp.bfloat16)

    slope, slopes, gains = input_backward(
        parity, own, other, query_own.reshape(NEAR, -1, tokens),
        query_other.reshape(NEAR, -1, tokens), x_turned, jnp.concatenate([mean, inv]), gain,
    )
    slopes = summed(slopes.reshape(8, 128), MP).reshape(2, tokens) / D
    input_gradient = (inv * (slope - slopes[0:1] - xhat * slopes[1:2])).astype(jnp.bfloat16).T

    gains = jnp.concatenate([gains[0], jnp.sum(qk_partial, axis=0)])
    gains = gains + swapped(gains.reshape(4, 128)).reshape(-1)
    rest = jnp.pad(thirds(gains).reshape(-1, rows), ((0, 4), (0, 0)))
    part = jnp.concatenate([part, jnp.broadcast_to(rest[None], (FAR, *rest.shape))], axis=1)
    part = exchange(part, "far")
    part = jnp.sum(part.astype(jnp.float32), axis=0)
    grad_weight = part[:COLS].T
    gains = jnp.sum(part[COLS : COLS + 4].reshape(3, 4, 128), axis=0)
    gains = jnp.sum(lax.all_gather(gains, ("high", "low"), axis=0), axis=0).reshape(-1)
    return (input_gradient, grad_weight, gains[:rows], gains[rows:])


def solution(mesh):
    finer = Mesh(mesh.devices.reshape(FAR, 2, 2, 2, 4, 4), (*DP, *MP))
    in_specs = (P(DP, MP), P(MP), P(MP, DP), P(DP, None), P(DP, None), P())
    out_specs = (P(DP, MP), P(MP, DP), P(MP), P())

    return jax.shard_map(
        shards, mesh=finer, in_specs=in_specs, out_specs=out_specs, check_vma=False
    )
```

```python
import jax
import jax.numpy as jnp
from jax import lax
from jax.experimental import pallas as pl
from jax.experimental.pallas import tpu as pltpu
from jax.sharding import Mesh
from jax.sharding import PartitionSpec as P


D = 6144
EPS = 1e-06
HEAD = 128
FAR, NEAR = 8, 4
COLS = 48
MP = ("x", "y")
DP = ("far", "high", "low", "core")


def qk_kernel(
    core_ref, query_ref, grad_ref, gain_ref, own_ref, other_ref, gain_grad_ref, rows_ref
):
    @pl.when(pl.program_id(0) == 0)
    def _():
        gain_grad_ref[...] = jnp.zeros_like(gain_grad_ref)

    core = core_ref[0]
    gain = gain_ref[...]
    scale = 1.0 / HEAD

    def three_heads(group, total):
        for j in range(3):
            cols = pl.ds(pl.multiple_of(group * 384 + j * HEAD, HEAD), HEAD)
            q = query_ref[:, cols].astype(jnp.float32)
            upstream = grad_ref[:, cols].astype(jnp.float32)
            mean = jnp.sum(q, axis=1, keepdims=True) * scale
            var = jnp.sum(q * q, axis=1, keepdims=True) * scale - mean * mean
            inv = lax.rsqrt(var + EPS)
            qhat = (q - mean) * inv
            dqhat = upstream * gain
            mean_d = jnp.sum(dqhat, axis=1, keepdims=True) * scale
            mean_c = jnp.sum(dqhat * qhat, axis=1, keepdims=True) * scale
            rows_ref[:, j * HEAD : (j + 1) * HEAD] = (
                inv * (dqhat - mean_d - qhat * mean_c)
            ).astype(jnp.bfloat16)
            total = total + jnp.sum((upstream * qhat).reshape(-1, 8, HEAD), axis=0)
        turned = jnp.transpose(rows_ref[...])
        for parity, (even_ref, odd_ref) in enumerate(((own_ref, other_ref), (other_ref, own_ref))):

            @pl.when(core == parity)
            def _():
                for b in range(8):
                    to_ref = odd_ref if b % 2 else even_ref
                    to_ref[b // 2, group] = turned[COLS * b : COLS * (b + 1)]

        return total

    zero = jnp.zeros((8, HEAD), jnp.float32)
    gain_grad_ref[...] += lax.fori_loop(0, FAR, three_heads, zero)


def qk_backward(core, query, grad_normed, qk_gain):
    tokens, width = query.shape
    block = 128
    return pl.pallas_call(
        qk_kernel,
        grid=(tokens // block,),
        in_specs=[
            pl.BlockSpec(memory_space=pltpu.SMEM),
            pl.BlockSpec((block, width), lambda i: (i, 0)),
            pl.BlockSpec((block, width), lambda i: (i, 0)),
            pl.BlockSpec((1, HEAD), lambda i: (0, 0)),
        ],
        out_specs=[
            pl.BlockSpec((NEAR, FAR, COLS, block), lambda i: (0, 0, 0, i)),
            pl.BlockSpec((NEAR, FAR, COLS, block), lambda i: (0, 0, 0, i)),
            pl.BlockSpec((8, HEAD), lambda i: (0, 0)),
        ],
        out_shape=[
            jax.ShapeDtypeStruct((NEAR, FAR, COLS, tokens), jnp.bfloat16),
            jax.ShapeDtypeStruct((NEAR, FAR, COLS, tokens), jnp.bfloat16),
            jax.ShapeDtypeStruct((8, HEAD), jnp.float32),
        ],
        scratch_shapes=[pltpu.VMEM((block, 3 * HEAD), jnp.bfloat16)],
        compiler_params=pltpu.CompilerParams(dimension_semantics=("arbitrary",)),
        cost_estimate=pl.CostEstimate(
            flops=60_000_000, bytes_accessed=9_500_000, transcendentals=12288
        ),
    )(core, query, grad_normed, qk_gain.reshape(1, HEAD))


def input_kernel(
    at_ref, own_ref, other_ref, query_own_ref, query_other_ref, x_ref, stat_ref, gain_ref,
    slope_ref, sums_ref, gains_ref, grad_ref,
):
    step = pl.program_id(0)

    def product(w_ref, q_ref):
        return lax.dot_general(
            w_ref[...], q_ref[0], (((0,), (0,)), ((), ())), preferred_element_type=jnp.float32
        )

    part = product(own_ref, query_own_ref) + product(other_ref, query_other_ref)

    @pl.when(step == 0)
    def _():
        grad_ref[...] = part

    @pl.when(step > 0)
    def _():
        grad_ref[...] += part

    @pl.when(step == NEAR - 1)
    def _():
        grad = grad_ref[...]
        xhat = (x_ref[...].astype(jnp.float32) - stat_ref[0:1]) * stat_ref[1:2]
        slope = grad * gain_ref[...]
        slope_ref[...] = slope
        sums_ref[0:1] = jnp.sum(slope, axis=0, keepdims=True)
        sums_ref[1:2] = jnp.sum(slope * xhat, axis=0, keepdims=True)
        cross = grad * xhat
        lanes = cross[:, :128] + cross[:, 128:256] + cross[:, 256:384] + cross[:, 384:]
        gains_ref[...] = jnp.sum(jnp.transpose(lanes), axis=0, keepdims=True)


def input_backward(at, own, other, query_own, query_other, x, stat, gain):
    rows, tokens = x.shape
    span = own.shape[0] // NEAR
    whole = lambda i, at: (0, 0)
    return pl.pallas_call(
        input_kernel,
        grid_spec=pltpu.PrefetchScalarGridSpec(
            num_scalar_prefetch=1,
            grid=(NEAR,),
            in_specs=[
                pl.BlockSpec((span, rows), lambda i, at: (i, 0)),
                pl.BlockSpec((span, rows), lambda i, at: (i, 0)),
                pl.BlockSpec((1, span, tokens), lambda i, at: (2 * (i % 2) + (at[0] + i // 2) % 2, 0, 0)),
                pl.BlockSpec((1, span, tokens), lambda i, at: (2 * (i % 2) + (at[0] + i // 2) % 2, 0, 0)),
                pl.BlockSpec((rows, tokens), whole),
                pl.BlockSpec((2, tokens), whole),
                pl.BlockSpec((rows, 1), whole),
            ],
            out_specs=[
                pl.BlockSpec((rows, tokens), whole),
                pl.BlockSpec((2, tokens), whole),
                pl.BlockSpec((1, rows), whole),
            ],
            scratch_shapes=[pltpu.VMEM((rows, tokens), jnp.float32)],
        ),
        out_shape=[
            jax.ShapeDtypeStruct((rows, tokens), jnp.float32),
            jax.ShapeDtypeStruct((2, tokens), jnp.float32),
            jax.ShapeDtypeStruct((1, rows), jnp.float32),
        ],
        compiler_params=pltpu.CompilerParams(dimension_semantics=("arbitrary",)),
        cost_estimate=pl.CostEstimate(
            flops=2_400_000_000, bytes_accessed=7_000_000, transcendentals=0
        ),
    )(at, own, other, query_own, query_other, x, stat, gain)


def exchange(x, axes):
    return lax.all_to_all(x, axes, 0, 0, tiled=True)


def shared_by(x, axes):
    copies = jnp.broadcast_to(x[None], (lax.axis_size(axes), *x.shape))
    return exchange(copies, axes)


def thirds(x):
    high = lax.reduce_precision(x, 8, 7)
    middle = lax.reduce_precision(x - high, 8, 7)
    return jnp.stack([high, middle, x - high - middle]).astype(jnp.bfloat16)


def summed(x, axes):
    for axis in axes:
        x = jnp.sum(lax.all_gather(x, axis, axis=0), axis=0)
    return x


def swapped(x):
    return lax.ppermute(x, "core", [(0, 1), (1, 0)])


def from_chip(x, distance):
    chips = FAR * NEAR
    return lax.ppermute(x, ("far", "high", "low"), [((i + distance) % chips, i) for i in range(chips)])


def shards(block_input, prenorm_gain, weight, query, grad_normed, qk_gain):
    tokens, rows = block_input.shape
    core = lax.axis_index("core").astype(jnp.int32)
    parity = lax.axis_index("low").astype(jnp.int32).reshape(1)

    own = lax.all_gather(weight.T, ("far", "high"), axis=0).reshape(FAR, 2, COLS, rows)
    even, odd = own[:, 0], own[:, 1]
    theirs_even = from_chip(even, 1)
    theirs_odd = from_chip(odd, -1)
    own = jnp.concatenate([even, odd, theirs_even, theirs_odd]).reshape(-1, rows)
    other = swapped(own)

    x_turned = block_input.T
    x = x_turned.astype(jnp.float32)
    sums = jnp.concatenate([jnp.sum(x, axis=0), jnp.sum(x * x, axis=0)]).reshape(8, 128)
    sums = shared_by(sums, MP)
    sums = jnp.sum(sums, axis=0).reshape(2, tokens)

    query_own, query_other, qk_partial = qk_backward(core.reshape(1), query, grad_normed, qk_gain)

    mean = sums[0:1] / D
    inv = lax.rsqrt(sums[1:2] / D - mean * mean + EPS)
    xhat = (x - mean) * inv
    gain = prenorm_gain[:, None]
    normed = (xhat * gain).astype(jnp.bfloat16)

    def weight_part(grad_query):
        return lax.dot_general(
            grad_query.reshape(-1, tokens), normed, (((1,), (1,)), ((), ())),
            preferred_element_type=jnp.float32,
        )

    part = weight_part(query_other).astype(jnp.bfloat16)
    from_core = swapped(part)
    part = weight_part(query_own) + from_core.astype(jnp.float32)
    part = part.astype(jnp.bfloat16).reshape(NEAR, FAR, COLS, rows)
    part = exchange(part, ("high", "low"))
    part = jnp.sum(part.astype(jnp.float32), axis=0).astype(jnp.bfloat16)

    slope, slopes, gains = input_backward(
        parity, own, other, query_own.reshape(NEAR, -1, tokens),
        query_other.reshape(NEAR, -1, tokens), x_turned, jnp.concatenate([mean, inv]), gain,
    )
    slopes = summed(slopes.reshape(8, 128), MP).reshape(2, tokens) / D
    input_gradient = (inv * (slope - slopes[0:1] - xhat * slopes[1:2])).astype(jnp.bfloat16).T

    gains = jnp.concatenate([gains[0], jnp.sum(qk_partial, axis=0)])
    gains = gains.reshape(4, 128)
    gains = gains + swapped(gains)
    gains = jnp.sum(lax.all_gather(gains, ("high", "low"), axis=0), axis=0).reshape(-1)
    rest = jnp.pad(thirds(gains).reshape(-1, rows), ((0, 4), (0, 0)))
    part = jnp.concatenate([part, jnp.broadcast_to(rest[None], (FAR, *rest.shape))], axis=1)
    part = exchange(part, "far")
    part = jnp.sum(part.astype(jnp.float32), axis=0)
    grad_weight = part[:COLS].T
    gains = jnp.sum(part[COLS : COLS + 4].reshape(3, -1), axis=0)
    return (input_gradient, grad_weight, gains[:rows], gains[rows:])


def solution(mesh):
    finer = Mesh(mesh.devices.reshape(FAR, 2, 2, 2, 4, 4), (*DP, *MP))
    in_specs = (P(DP, MP), P(MP), P(MP, DP), P(DP, None), P(DP, None), P())
    out_specs = (P(DP, MP), P(MP, DP), P(MP), P())

    return jax.shard_map(
        shards, mesh=finer, in_specs=in_specs, out_specs=out_specs, check_vma=False
    )
```

```python
import jax
import jax.numpy as jnp
from jax import lax
from jax.experimental import pallas as pl
from jax.experimental.pallas import tpu as pltpu
from jax.sharding import Mesh
from jax.sharding import PartitionSpec as P


D = 6144
EPS = 1e-06
HEAD = 128
FAR, NEAR = 8, 4
COLS = 48
MP = ("x", "y")
DP = ("far", "high", "low", "core")


def qk_kernel(
    core_ref, query_ref, grad_ref, gain_ref, own_ref, other_ref, gain_grad_ref, rows_ref
):
    @pl.when(pl.program_id(0) == 0)
    def _():
        gain_grad_ref[...] = jnp.zeros_like(gain_grad_ref)

    core = core_ref[0]
    gain = gain_ref[...]
    scale = 1.0 / HEAD

    def three_heads(group, total):
        for j in range(3):
            cols = pl.ds(pl.multiple_of(group * 384 + j * HEAD, HEAD), HEAD)
            for r in range(0, query_ref.shape[0], 32):
                at = pl.ds(r, 32)
                q = query_ref[at, cols].astype(jnp.float32)
                upstream = grad_ref[at, cols].astype(jnp.float32)
                dqhat = upstream * gain
                mean = jnp.sum(q, axis=1, keepdims=True) * scale
                mean_d = jnp.sum(dqhat, axis=1, keepdims=True) * scale
                square = jnp.sum(q * q, axis=1, keepdims=True) * scale
                cross = jnp.sum(dqhat * q, axis=1, keepdims=True) * scale
                inv = lax.rsqrt(square - mean * mean + EPS)
                mean_c = (cross - mean * mean_d) * inv
                qhat = (q - mean) * inv
                rows_ref[at, j * HEAD : (j + 1) * HEAD] = (
                    inv * (dqhat - mean_d - qhat * mean_c)
                ).astype(jnp.bfloat16)
                total = total + jnp.sum((upstream * qhat).reshape(-1, 8, HEAD), axis=0)
        turned = jnp.transpose(rows_ref[...])
        for parity, (even_ref, odd_ref) in enumerate(((own_ref, other_ref), (other_ref, own_ref))):

            @pl.when(core == parity)
            def _():
                for b in range(8):
                    to_ref = odd_ref if b % 2 else even_ref
                    to_ref[b // 2, group] = turned[COLS * b : COLS * (b + 1)]

        return total

    zero = jnp.zeros((8, HEAD), jnp.float32)
    gain_grad_ref[...] += lax.fori_loop(0, FAR, three_heads, zero)


def qk_backward(core, query, grad_normed, qk_gain):
    tokens, width = query.shape
    block = 128
    return pl.pallas_call(
        qk_kernel,
        grid=(tokens // block,),
        in_specs=[
            pl.BlockSpec(memory_space=pltpu.SMEM),
            pl.BlockSpec((block, width), lambda i: (i, 0)),
            pl.BlockSpec((block, width), lambda i: (i, 0)),
            pl.BlockSpec((1, HEAD), lambda i: (0, 0)),
        ],
        out_specs=[
            pl.BlockSpec((NEAR, FAR, COLS, block), lambda i: (0, 0, 0, i)),
            pl.BlockSpec((NEAR, FAR, COLS, block), lambda i: (0, 0, 0, i)),
            pl.BlockSpec((8, HEAD), lambda i: (0, 0)),
        ],
        out_shape=[
            jax.ShapeDtypeStruct((NEAR, FAR, COLS, tokens), jnp.bfloat16),
            jax.ShapeDtypeStruct((NEAR, FAR, COLS, tokens), jnp.bfloat16),
            jax.ShapeDtypeStruct((8, HEAD), jnp.float32),
        ],
        scratch_shapes=[pltpu.VMEM((block, 3 * HEAD), jnp.bfloat16)],
        compiler_params=pltpu.CompilerParams(dimension_semantics=("arbitrary",)),
        cost_estimate=pl.CostEstimate(
            flops=60_000_000, bytes_accessed=9_500_000, transcendentals=12288
        ),
    )(core, query, grad_normed, qk_gain.reshape(1, HEAD))


def input_kernel(
    at_ref, own_ref, other_ref, query_own_ref, query_other_ref, x_ref, stat_ref, gain_ref,
    slope_ref, sums_ref, gains_ref, grad_ref,
):
    step = pl.program_id(0)

    def product(w_ref, q_ref):
        return lax.dot_general(
            w_ref[...], q_ref[0], (((0,), (0,)), ((), ())), preferred_element_type=jnp.float32
        )

    part = product(own_ref, query_own_ref) + product(other_ref, query_other_ref)

    @pl.when(step == 0)
    def _():
        grad_ref[...] = part

    @pl.when(step > 0)
    def _():
        grad_ref[...] += part

    @pl.when(step == NEAR - 1)
    def _():
        grad = grad_ref[...]
        xhat = (x_ref[...].astype(jnp.float32) - stat_ref[0:1]) * stat_ref[1:2]
        slope = grad * gain_ref[...]
        slope_ref[...] = slope
        sums_ref[0:1] = jnp.sum(slope, axis=0, keepdims=True)
        sums_ref[1:2] = jnp.sum(slope * xhat, axis=0, keepdims=True)
        cross = grad * xhat
        lanes = cross[:, :128] + cross[:, 128:256] + cross[:, 256:384] + cross[:, 384:]
        gains_ref[...] = jnp.sum(jnp.transpose(lanes), axis=0, keepdims=True)


def input_backward(at, own, other, query_own, query_other, x, stat, gain):
    rows, tokens = x.shape
    span = own.shape[0] // NEAR
    whole = lambda i, at: (0, 0)
    return pl.pallas_call(
        input_kernel,
        grid_spec=pltpu.PrefetchScalarGridSpec(
            num_scalar_prefetch=1,
            grid=(NEAR,),
            in_specs=[
                pl.BlockSpec((span, rows), lambda i, at: (i, 0)),
                pl.BlockSpec((span, rows), lambda i, at: (i, 0)),
                pl.BlockSpec((1, span, tokens), lambda i, at: (2 * (i % 2) + (at[0] + i // 2) % 2, 0, 0)),
                pl.BlockSpec((1, span, tokens), lambda i, at: (2 * (i % 2) + (at[0] + i // 2) % 2, 0, 0)),
                pl.BlockSpec((rows, tokens), whole),
                pl.BlockSpec((2, tokens), whole),
                pl.BlockSpec((rows, 1), whole),
            ],
            out_specs=[
                pl.BlockSpec((rows, tokens), whole),
                pl.BlockSpec((2, tokens), whole),
                pl.BlockSpec((1, rows), whole),
            ],
            scratch_shapes=[pltpu.VMEM((rows, tokens), jnp.float32)],
        ),
        out_shape=[
            jax.ShapeDtypeStruct((rows, tokens), jnp.float32),
            jax.ShapeDtypeStruct((2, tokens), jnp.float32),
            jax.ShapeDtypeStruct((1, rows), jnp.float32),
        ],
        compiler_params=pltpu.CompilerParams(dimension_semantics=("arbitrary",)),
        cost_estimate=pl.CostEstimate(
            flops=2_400_000_000, bytes_accessed=7_000_000, transcendentals=0
        ),
    )(at, own, other, query_own, query_other, x, stat, gain)


def exchange(x, axes):
    return lax.all_to_all(x, axes, 0, 0, tiled=True)


def shared_by(x, axes):
    copies = jnp.broadcast_to(x[None], (lax.axis_size(axes), *x.shape))
    return exchange(copies, axes)


def thirds(x):
    high = lax.reduce_precision(x, 8, 7)
    middle = lax.reduce_precision(x - high, 8, 7)
    return jnp.stack([high, middle, x - high - middle]).astype(jnp.bfloat16)


def summed(x, axes):
    for axis in axes:
        x = jnp.sum(lax.all_gather(x, axis, axis=0), axis=0)
    return x


def swapped(x):
    return lax.ppermute(x, "core", [(0, 1), (1, 0)])


def from_chip(x, distance):
    chips = FAR * NEAR
    return lax.ppermute(x, ("far", "high", "low"), [((i + distance) % chips, i) for i in range(chips)])


def shards(block_input, prenorm_gain, weight, query, grad_normed, qk_gain):
    tokens, rows = block_input.shape
    core = lax.axis_index("core").astype(jnp.int32)
    parity = lax.axis_index("low").astype(jnp.int32).reshape(1)

    own = lax.all_gather(weight.T, ("far", "high"), axis=0).reshape(FAR, 2, COLS, rows)
    even, odd = own[:, 0], own[:, 1]
    theirs_even = from_chip(even, 1)
    theirs_odd = from_chip(odd, -1)
    own = jnp.concatenate([even, odd, theirs_even, theirs_odd]).reshape(-1, rows)
    other = swapped(own)

    x_turned = block_input.T
    x = x_turned.astype(jnp.float32)
    sums = jnp.concatenate([jnp.sum(x, axis=0), jnp.sum(x * x, axis=0)]).reshape(8, 128)
    sums = shared_by(sums, MP)
    sums = jnp.sum(sums, axis=0).reshape(2, tokens)

    query_own, query_other, qk_partial = qk_backward(core.reshape(1), query, grad_normed, qk_gain)

    mean = sums[0:1] / D
    inv = lax.rsqrt(sums[1:2] / D - mean * mean + EPS)
    xhat = (x - mean) * inv
    gain = prenorm_gain[:, None]
    normed = (xhat * gain).astype(jnp.bfloat16)

    def weight_part(grad_query):
        return lax.dot_general(
            grad_query.reshape(-1, tokens), normed, (((1,), (1,)), ((), ())),
            preferred_element_type=jnp.float32,
        )

    part = weight_part(query_other).astype(jnp.bfloat16)
    from_core = swapped(part)
    part = weight_part(query_own) + from_core.astype(jnp.float32)
    part = part.astype(jnp.bfloat16).reshape(NEAR, FAR, COLS, rows)
    part = exchange(part, ("high", "low"))
    part = jnp.sum(part.astype(jnp.float32), axis=0).astype(jnp.bfloat16)

    slope, slopes, gains = input_backward(
        parity, own, other, query_own.reshape(NEAR, -1, tokens),
        query_other.reshape(NEAR, -1, tokens), x_turned, jnp.concatenate([mean, inv]), gain,
    )
    slopes = summed(slopes.reshape(8, 128), MP).reshape(2, tokens) / D
    input_gradient = (inv * (slope - slopes[0:1] - xhat * slopes[1:2])).astype(jnp.bfloat16).T

    gains = jnp.concatenate([gains[0], jnp.sum(qk_partial, axis=0)])
    gains = gains.reshape(4, 128)
    gains = gains + swapped(gains)
    gains = jnp.sum(lax.all_gather(gains, ("high", "low"), axis=0), axis=0).reshape(-1)
    rest = jnp.pad(thirds(gains).reshape(-1, rows), ((0, 4), (0, 0)))
    part = jnp.concatenate([part, jnp.broadcast_to(rest[None], (FAR, *rest.shape))], axis=1)
    part = exchange(part, "far")
    part = jnp.sum(part.astype(jnp.float32), axis=0)
    grad_weight = part[:COLS].T
    gains = jnp.sum(part[COLS : COLS + 4].reshape(3, -1), axis=0)
    return (input_gradient, grad_weight, gains[:rows], gains[rows:])


def solution(mesh):
    finer = Mesh(mesh.devices.reshape(FAR, 2, 2, 2, 4, 4), (*DP, *MP))
    in_specs = (P(DP, MP), P(MP), P(MP, DP), P(DP, None), P(DP, None), P())
    out_specs = (P(DP, MP), P(MP, DP), P(MP), P())

    return jax.shard_map(
        shards, mesh=finer, in_specs=in_specs, out_specs=out_specs, check_vma=False
    )
```
